32 devices in a mesh: blk: 8 (over z, x), grp: 4 (over y, core).
Axes of the slice: x: 2, y: 2, z: 4, core: 2. Of those that a mesh axis runs over, the one named last changes fastest.
Arguments:
- sources: bfloat16 [8192, 256], P('blk'), may hold values from -64 to 64
- positive: int32 [8192], P('blk'), may hold values from 0 to 8191
- src_part: int32 [8192], P('blk'), may hold values from 0 to 7
- destinations: bfloat16 [8192, 256], P(('blk', 'grp')), may hold values from -8 to 8
- dst_part: int32 [8192], P(('blk', 'grp')), may hold values from 0 to 7
Outputs:
- loss: float32 [8192], P('blk')
The draws below stay inside these ranges and needn't reach their ends.
All inputs are finite; a program needn't handle non-finite values.
Results may differ from the reference program's by a relative error of at most 0.0003.
Values may be sent and summed in bfloat16 or wider, within the bound.
No kernel may reach another device: no remote copies, remote signals or barrier semaphores. Data moves between devices by JAX's collectives and lax.ppermute only.
A program may use at most 192 MiB of HBM per device.

```python
import jax
import jax.numpy as jnp
from jax import lax

H = 256
SRC_DEV = 1024
PARTS_SIZE = 8
NSRC = 8192
NDST = 8192
N_BLK = 8


def joint_draw(key):
    keys = jax.random.split(jax.random.fold_in(key, 7), 2)
    src = jax.random.normal(keys[0], (NSRC, H), jnp.float32)
    dst = jax.random.normal(keys[1], (NDST, H), jnp.float32) * H ** (-0.5)
    return (jnp.clip(src, -64.0, 64.0), jnp.clip(dst, -8.0, 8.0))


def draw_sources(key, part):
    return joint_draw(key)[0].astype(jnp.bfloat16)


def draw_destinations(key, part):
    return joint_draw(key)[1].astype(jnp.bfloat16)


def touch_ends(result, own_key, smallest, largest):
    longest = result.shape.index(max(result.shape))
    spots = []
    for shift in (0, 1):
        where = [jax.random.randint(jax.random.fold_in(own_key, axis), (), 0, length) for axis, length in enumerate(result.shape)]
        where[longest] = (where[longest] + shift) % result.shape[longest]
        spots.append(tuple(where))
    return result.at[spots[0]].set(smallest).at[spots[1]].set(largest)


def setup_inputs(seed: int = 0) -> dict:
    key_list = jax.random.split(jax.random.key(seed), 6)
    sources = draw_sources(jax.random.fold_in(key_list[5], 71), 0)
    positive = touch_ends(jax.random.randint(key_list[1], (NSRC,), 0, NDST), jax.random.fold_in(key_list[1], 1), 0, NDST - 1).astype(jnp.int32)
    src_part = touch_ends(jax.random.randint(key_list[2], (NSRC,), 0, PARTS_SIZE), jax.random.fold_in(key_list[2], 1), 0, PARTS_SIZE - 1).astype(jnp.int32)
    destinations = draw_destinations(jax.random.fold_in(key_list[5], 71), 0)
    dst_part = touch_ends(jax.random.randint(key_list[4], (NDST,), 0, PARTS_SIZE), jax.random.fold_in(key_list[4], 1), 0, PARTS_SIZE - 1).astype(jnp.int32)
    return dict(sources=sources, positive=positive, src_part=src_part, destinations=destinations, dst_part=dst_part)


SCALE = 3.0
NEG = -1.0e30


def reference(sources, positive, src_part, destinations, dst_part):
    columns = jnp.arange(NDST, dtype=jnp.int32)
    src_blocks = sources.reshape(N_BLK, SRC_DEV, H)
    pos_blocks = positive.reshape(N_BLK, SRC_DEV)
    part_blocks = src_part.reshape(N_BLK, SRC_DEV)

    def one_block(item):
        rows, pos, part = item
        logits = SCALE * lax.dot_general(rows, destinations, (((1,), (1,)), ((), ())), preferred_element_type=jnp.float32)
        is_pos = columns[None, :] == pos[:, None]
        keep = (dst_part[None, :] != part[:, None]) | is_pos
        masked = jnp.where(keep, logits, NEG)
        top = jnp.max(masked, axis=1)
        total = jnp.sum(jnp.where(keep, jnp.exp(masked - top[:, None]), jnp.float32(0.0)), axis=1)
        pos_logit = jnp.sum(jnp.where(is_pos, logits, jnp.float32(0.0)), axis=1)
        return top + jnp.log(total) - pos_logit

    losses = lax.map(one_block, (src_blocks, pos_blocks, part_blocks))
    return losses.reshape(NSRC)
```

```python
import functools

import jax
import jax.numpy as jnp
from jax import lax
from jax.experimental import pallas as pl
from jax.experimental.pallas import tpu as pltpu
from jax.sharding import PartitionSpec as P


SCALE = 3.0
NEG = -1e30
RATE = SCALE * 1.4426950408889634
LANES = 128
SUB = 8
CHUNK = 2 * LANES
AXES = ("blk", "grp")
VM = pl.BlockSpec(memory_space=pltpu.VMEM)
HB = pl.BlockSpec(memory_space=pltpu.HBM)


def tree(join, values):
    values = list(values)
    while len(values) > 1:
        values = [functools.reduce(join, values[k : k + 2]) for k in range(0, len(values), 2)]
    return values[0]


def call(body, out_shape, operands, scratch=(), flops=0, exps=0, space=VM):
    moved = sum(v.size * v.dtype.itemsize for v in [*operands, *jax.tree.leaves(out_shape)])
    return pl.pallas_call(
        body,
        out_shape=out_shape,
        in_specs=[space] * len(operands),
        out_specs=jax.tree.map(lambda _: VM, out_shape),
        scratch_shapes=list(scratch),
        compiler_params=pltpu.CompilerParams(vmem_limit_bytes=16 << 20),
        cost_estimate=pl.CostEstimate(flops=flops, transcendentals=exps, bytes_accessed=moved),
    )(*operands)


def prepare_body(destinations, dst_part, positive, src_part, packed, ids, parts, sems):
    rows = destinations.shape[0]
    half = positive.shape[0]
    moves = [
        (dst_part, parts),
        (destinations, packed.at[0:rows, :]),
        (positive, ids.at[0:half, :]),
        (src_part, ids.at[half : 2 * half, :]),
    ]
    copies = [pltpu.make_async_copy(*move, sems.at[k]) for k, move in enumerate(moves)]
    for copy in copies:
        copy.start()
    copies[0].wait()
    line = jnp.concatenate([parts[r : r + 1, :] for r in range(parts.shape[0])], axis=1)
    packed[rows : rows + SUB, :] = jnp.broadcast_to(line.astype(jnp.float32), (SUB, line.shape[1])).astype(packed.dtype)
    for copy in copies[1:]:
        copy.wait()


def set_column(piece, column, rows):
    line = piece[rows : rows + SUB, :].astype(jnp.float32)[0:1, :]
    for t in range(0, rows, LANES):
        column[t : t + LANES, :] = jnp.broadcast_to(line[:, t : t + LANES], (LANES, LANES)).T


def lane_group(logits, lane, column, row_ids, pos, part, carry):
    top, total, found = carry
    kept = []
    for t in range(0, logits.shape[0], SUB):
        x = logits[t : t + SUB, lane : lane + LANES]
        is_pos = row_ids[t : t + SUB, :] == pos
        found = jnp.where(is_pos, x, found)
        kept.append(jnp.where(is_pos, x, jnp.where(column[t : t + SUB, :] == part, NEG, x)))
    new = jnp.maximum(top, tree(jnp.maximum, kept))
    total = total * jnp.exp2((top - new) * RATE) + tree(jnp.add, [jnp.exp2((x - new) * RATE) for x in kept])
    return new, total, found


def fold_block(pieces, bases, columns, row_ids, block, before, finish):
    sources, ids = block
    count = sources.shape[0]
    rows = row_ids.shape[0]
    for i in range(0, count, CHUNK):
        logits = [
            lax.dot_general(
                piece[0:rows, :],
                sources[i : i + CHUNK, :],
                (((1,), (1,)), ((), ())),
                preferred_element_type=jnp.float32,
            )
            for piece in pieces
        ]
        for lane in range(0, CHUNK, LANES):
            g = (i + lane) // LANES
            h = count // LANES + g
            here = slice(i + lane, i + lane + LANES)
            part = jnp.broadcast_to(ids[h : h + 1, :], (SUB, LANES)).astype(jnp.float32)
            if before is None:
                carry = (jnp.full((SUB, LANES), NEG, jnp.float32),) + (jnp.zeros((SUB, LANES), jnp.float32),) * 2
            else:
                carry = tuple(before[SUB * r : SUB * (r + 1), here] for r in range(3))
            for p, base in enumerate(bases):
                pos = jnp.broadcast_to(ids[g : g + 1, :] - base, (SUB, LANES))
                carry = lane_group(logits[p], lane, columns.at[p], row_ids, pos, part, carry)
            finish(here, *carry)


def place():
    here = lax.axis_index("blk")
    return here // 2, here % 2, lax.axis_index("grp")


def base_of(z, rows):
    _, side, group = place()
    return ((z * 2 + side) * lax.axis_size("grp") + group) * rows


def pick(block, chosen=None):
    if len(block) == 2:
        return block
    group = place()[2]
    chosen[...] = jnp.where(group % 2 == 1, block[0][...], block[1][...])
    return chosen, block[2]


def gather_body(origins, n_block, resumed, *refs):
    n = len(origins)
    pieces, block = refs[:n], refs[n : n + n_block]
    before = refs[n + n_block] if resumed else None
    out, columns, row_ids, *chosen = refs[n + n_block + resumed :]
    rows = row_ids.shape[0]
    row_ids[...] = lax.broadcasted_iota(jnp.int32, row_ids.shape, 0)
    for p in range(n):
        set_column(pieces[p], columns.at[p], rows)

    def finish(here, *carry):
        for r, value in enumerate(carry):
            out[SUB * r : SUB * (r + 1), here] = value

    bases = [base_of(origin(place()[0]), rows) for origin in origins]
    fold_block(pieces, bases, columns, row_ids, pick(block, *chosen), before, finish)


def last_body(origin, outer, inner, own, own_ids, far, far_south, far_ids, own_before, far_before, out, *scratch):
    columns, row_ids, chosen, piece = scratch
    rows = row_ids.shape[0]
    spot = place()[0]
    ends = (spot == 0) | (spot == lax.axis_size("blk") // 2 - 1)
    piece[...] = jnp.where(ends, outer[...], inner[...])
    row_ids[...] = lax.broadcasted_iota(jnp.int32, row_ids.shape, 0)
    set_column(piece, columns.at[0], rows)
    blocks = (((own, own_ids), own_before), (pick((far, far_south, far_ids), chosen), far_before))
    for k, (block, before) in enumerate(blocks):

        def finish(here, top, total, found, k=k):
            peak = jnp.max(top, axis=0, keepdims=True)
            out[3 * k : 3 * k + 1, here] = peak
            out[3 * k + 1 : 3 * k + 2, here] = jnp.sum(
                total * jnp.exp2((top - peak) * RATE), axis=0, keepdims=True
            )
            out[3 * k + 2 : 3 * k + 3, here] = jnp.sum(found, axis=0, keepdims=True)

        fold_block([piece], [base_of(origin(spot), rows)], columns, row_ids, block, before, finish)


def joined(parts):
    peak = tree(jnp.maximum, [p[0] for p in parts])
    total = tree(jnp.add, [p[1] * jnp.exp2((p[0] - peak) * RATE) for p in parts])
    return peak, total, tree(jnp.add, [p[2] for p in parts])


def pair_body(mine, other, own_out, far_out):
    for k, out in ((0, own_out), (1, far_out)):
        parts = [tuple(v[3 * k + r : 3 * k + r + 1, :] for r in range(3)) for v in (mine, other)]
        for r, value in enumerate(joined(parts)):
            out[r : r + 1, :] = value


def final_body(*refs):
    out = refs[-1]
    peak, total, found = joined([tuple(ref[r : r + 1, :] for r in range(3)) for ref in refs[:-1]])
    loss = (peak - found) * SCALE + jnp.log(total)
    for i in range(out.shape[0]):
        out[i : i + 1, :] = loss[:, i * LANES : (i + 1) * LANES]


NEAR = {0: 2, 3: 1, 1: 0, 2: 3}
CROSS = {0: 1, 3: 2, 1: 3, 2: 0}
RELAY = {1: 0, 2: 3}


def source_of(route):
    return lambda z: sum(jnp.where(z == t, s, 0) for s, t in route.items())


def device_body(sources, positive, src_part, destinations, dst_part):
    rows, width = destinations.shape
    count = sources.shape[0]
    groups = lax.axis_size("grp")
    cycle = lax.axis_size("blk")
    line = cycle // 2

    def sent(value, move, take=lambda b, g: True):
        route = []
        for b in range(cycle):
            for g in range(groups):
                target = move(b // 2, b % 2, g) if take(b, g) else None
                if target is not None:
                    z, x, h = target
                    route.append((b * groups + g, (z * 2 + x) * groups + h))
        return lax.ppermute(value, AXES, route)

    def tiles(v):
        return v.reshape(-1, LANES)

    def shape(*dims):
        return jax.ShapeDtypeStruct(dims, jnp.float32)

    packed, ids = call(
        prepare_body,
        [
            jax.ShapeDtypeStruct((rows + SUB, width), destinations.dtype),
            jax.ShapeDtypeStruct((2 * count // LANES, LANES), jnp.int32),
        ],
        [destinations, tiles(dst_part), tiles(positive), tiles(src_part)],
        scratch=[pltpu.VMEM((rows // LANES, LANES), jnp.int32), pltpu.SemaphoreType.DMA((4,))],
        space=HB,
    )
    far = sent(sources, lambda z, x, g: (z, 1 - x, g), lambda b, g: g % 2 == 1)
    far_ids = sent(ids, lambda z, x, g: (z, 1 - x, g))
    far_south = sent(far, lambda z, x, g: (z, x, g - 1), lambda b, g: g % 2 == 1)
    block_copy = pltpu.VMEM(sources.shape, sources.dtype)

    def scratch(n):
        return [pltpu.VMEM((n, rows, LANES), jnp.float32), pltpu.VMEM((rows, LANES), jnp.int32)]

    def cost(n):
        return dict(flops=2 * n * rows * count * width, exps=n * rows * count)

    def gather(origins, pieces, block, before=None):
        return call(
            functools.partial(gather_body, origins, len(block), int(before is not None)),
            shape(3 * SUB, count),
            [*pieces, *block] + ([] if before is None else [before]),
            scratch(len(pieces)) + [block_copy] * (len(block) == 3),
            **cost(len(pieces)),
        )

    own_block = (sources, ids)
    far_block = (far, far_south, far_ids)
    mine = lambda z: z
    if line == 4:
        first = sent(packed, lambda z, x, g: (NEAR[z], x, g))
        second = sent(packed, lambda z, x, g: (CROSS[z], x, g))
        inner = sent(packed, lambda z, x, g: (3 - z, x, g) if z in RELAY else None)
        outer = sent(first, lambda z, x, g: (RELAY[z], x, g) if z in RELAY else None)
        from_first, from_second, origin = source_of(NEAR), source_of(CROSS), lambda z: line - 1 - z
        own_state = gather([mine], [packed], own_block)
        own_state = gather([from_first, from_second], [first, second], own_block, own_state)
        far_state = gather([mine, from_first, from_second], [packed, first, second], far_block)
    else:
        def turn(step, state):
            piece, own_state, far_state = state
            piece = sent(piece, lambda z, x, g: ((z + 1) % line, x, g))
            origin = [lambda z: (z - step) % line]
            own_state = gather(origin, [piece], own_block, own_state)
            far_state = gather(origin, [piece], far_block, far_state)
            return piece, own_state, far_state

        states = (gather([mine], [packed], own_block), gather([mine], [packed], far_block))
        state = (packed, *states)
        for step in range(1, line - 1):
            state = turn(step, state)
        outer, own_state, far_state = state
        outer = inner = sent(outer, lambda z, x, g: ((z + 1) % line, x, g))
        origin = lambda z: (z + 1) % line
    partial = call(
        functools.partial(last_body, origin),
        shape(8, count),
        [outer, inner, sources, ids, far, far_south, far_ids, own_state, far_state],
        scratch(1) + [block_copy, pltpu.VMEM(packed.shape, packed.dtype)],
        **cost(2),
    )
    partner = sent(partial, lambda z, x, g: (z, x, g ^ 1))
    near_sum, far_sum = call(pair_body, [shape(3, count)] * 2, [partial, partner])
    gathered = [near_sum]
    for hop in range(0, groups, 2):
        for flip in (1, 0):
            if hop or flip:
                value = far_sum if flip else near_sum
                gathered.append(sent(value, lambda z, x, g: (z, x ^ flip, g ^ hop)))
    loss = call(final_body, shape(count // LANES, LANES), gathered)
    return loss.reshape(count)


def solution(mesh):
    return jax.shard_map(
        device_body,
        mesh=mesh,
        in_specs=(P("blk", None), P("blk"), P("blk"), P(("blk", "grp"), None), P(("blk", "grp"))),
        out_specs=P("blk"),
        check_vma=False,
    )
```
